32 devices in a mesh: feat: 4 (over y, core), dom: 8 (over z, x).
Axes of the slice: x: 2, y: 2, z: 4, core: 2. Of those that a mesh axis runs over, the one named last changes fastest.
Arguments:
- features: bfloat16 [32768, 128], P('dom'), may hold values from -6 to 6
- w_input: bfloat16 [128, 256], P(None, 'feat'), may hold values from -0.5 to 0.5
- layer_weights: bfloat16 [4, 256, 256], replicated, may hold values from -0.375 to 0.375
- history: bfloat16 [4, 32768, 256], P(None, 'dom', 'feat'), may hold values from 0 to 2
- tile_values: bfloat16 [256, 6, 128, 128], P('dom'), may hold values from -0.21875 to 0.21875
- tile_columns: int32 [256, 6], P('dom'), may hold values from 0 to 63, as said below
- send_rows: int32 [8, 8, 512], P('dom'), may hold values from 0 to 4095
- send_counts: int32 [8, 8], P('dom'), may hold values from 0 to 512, as said below
Outputs:
- pushed: bfloat16 [4, 32768, 256], P(None, 'dom', 'feat')
- final_rows: bfloat16 [32768, 256], P('dom', 'feat')
The draws below stay inside these ranges and needn't reach their ends.
Inputs may be any that keep to these rules, and one draw needn't show every extreme that they name: `tile_columns`: per row of tiles the first 2 entries lie below 4096 / 128 (own rows), the others at or above it (halo slots); every halo column tile of every partition is named somewhere. `send_counts`: A partition sends nothing to itself; in every draw some destination receives exactly 512 rows from every other partition.
All inputs are finite; a program needn't handle non-finite values.
Results may differ from the reference program's by a relative error of at most 0.0052.
Values may be sent and summed in bfloat16 or wider, within the bound.
A program may use at most 128 MiB of HBM per device.

```python
import math
import jax
import jax.numpy as jnp
from jax import lax

F = 256
IN_FEAT = 128
NODES_DEV = 4096
CAP = 512
TILE = 128
K = 6
K_LOC = 2
LAYERS = 4
NODES = 32768
HALO = 4096
ROW_TILES = 256
N_DOM = 8


def shuffle_one(sub_key, span):
    return jax.random.permutation(sub_key, span)


def draw_tile_columns(key, part):
    local_tiles = NODES_DEV // TILE
    halo_tiles = HALO // TILE
    remote_count = K - K_LOC
    key_local, key_shuffle = jax.random.split(key)
    local_cols = jax.random.randint(key_local, (ROW_TILES, K_LOC), 0, local_tiles)
    block_keys = jax.random.split(key_shuffle, N_DOM)
    span = local_tiles * remote_count
    shuffled = jax.vmap(lambda sub_key: shuffle_one(sub_key, span))(block_keys)
    remote = local_tiles + shuffled % halo_tiles
    remote = remote.reshape(ROW_TILES, remote_count)
    return jnp.concatenate([local_cols, remote], axis=1).astype(jnp.int32)


def draw_send_counts(key, part):
    key_heavy, key_high, key_low, key_busy = jax.random.split(key, 4)
    dest_ids = jnp.arange(N_DOM)
    busiest = jax.random.randint(key_busy, (), 0, N_DOM)
    heavy_dest = (jax.random.randint(key_heavy, (N_DOM,), 0, 4) == 0) | (dest_ids == busiest)
    high_counts = jax.random.randint(key_high, (N_DOM, N_DOM), CAP // 2, CAP + 1)
    low_counts = jax.random.randint(key_low, (N_DOM, N_DOM), (CAP + 7) // 8, CAP // 2 + 1)
    counts = jnp.where(heavy_dest[None, :], high_counts, low_counts)
    counts = jnp.where(dest_ids[None, :] == busiest, CAP, counts)
    counts = jnp.where(dest_ids[:, None] == dest_ids[None, :], 0, counts)
    return counts.astype(jnp.int32)


def touch_ends(drawn, rng, low, top_value):
    place = [jax.random.randint(jax.random.fold_in(rng, axis), (), 0, length) for axis, length in enumerate(drawn.shape)]
    main_axis = drawn.shape.index(max(drawn.shape))
    neighbour = place[:main_axis] + [(place[main_axis] + 1) % drawn.shape[main_axis]] + place[main_axis + 1:]
    return drawn.at[tuple(place)].set(low).at[tuple(neighbour)].set(top_value)


def shard_levels(rng, extent, shards, least, largest):
    gain = 1.0
    for dim, parts in shards:
        draws = jax.random.uniform(jax.random.fold_in(jax.random.fold_in(rng, 6), dim), (parts,), jnp.float32, least / len(shards), largest / len(shards))
        gain = gain * jnp.repeat(jnp.exp(draws), extent[dim] // parts).reshape((-1,) + (1,) * (len(extent) - 1 - dim))
    return gain


def normal_values(key, dims, spread, reach, pieces=(), kind=jnp.bfloat16):
    drawn = jax.random.normal(key, dims, jnp.float32) * spread
    if len(pieces) > 0:
        drawn = shard_levels(key, dims, pieces, -0.22, 0.18) * drawn
    return jnp.clip(drawn, min=-reach, max=reach).astype(kind)


def setup_inputs(seed: int = 0) -> dict:
    splits = jax.random.split(jax.random.key(seed), 9)
    features = normal_values(splits[0], (NODES, IN_FEAT), 1.0, 6.0, ((0, 8),))
    w_input = normal_values(splits[1], (IN_FEAT, F), IN_FEAT ** -0.5, 0.5, ((1, 4),))
    layer_weights = normal_values(splits[2], (LAYERS, F, F), F ** -0.5, 0.375)
    history = jnp.clip(2.0 * jax.random.uniform(splits[3], (LAYERS, NODES, F), jnp.float32) ** shard_levels(splits[3], (LAYERS, NODES, F), ((1, 8), (2, 4)), -0.2, 0.2), 0.0, 2.0).astype(jnp.bfloat16)
    tile_values = normal_values(splits[4], (ROW_TILES, K, TILE, TILE), (K * TILE) ** -0.5, 0.21875, ((0, 8),))
    tile_columns = draw_tile_columns(jax.random.fold_in(splits[8], 71), 0)
    send_rows = touch_ends(jax.random.randint(splits[6], (N_DOM, N_DOM, CAP), 0, NODES_DEV), jax.random.fold_in(splits[6], 1), 0, NODES_DEV - 1).astype(jnp.int32)
    send_counts = draw_send_counts(jax.random.fold_in(splits[8], 71), 0)
    return dict(features=features, w_input=w_input, layer_weights=layer_weights, history=history, tile_values=tile_values, tile_columns=tile_columns, send_rows=send_rows, send_counts=send_counts)


ALPHA = 0.1
LAMBDA_DECAY = 0.5


def reference(features, w_input, layer_weights, history, tile_values, tile_columns, send_rows, send_counts):
    initial = jnp.maximum(jnp.dot(features, w_input, preferred_element_type=jnp.float32), 0.0).astype(jnp.bfloat16)
    slot_ids = jnp.arange(CAP)
    sources = jnp.arange(N_DOM)
    local_tiles = NODES_DEV // TILE
    pushed = []
    current = initial
    for layer_index in range(LAYERS):
        beta_layer = math.log(LAMBDA_DECAY / (layer_index + 1) + 1.0)
        layer_table = history[layer_index]

        def one_part(part_index):
            source_rows = sources[:, None] * NODES_DEV + send_rows[:, part_index, :]
            live_mask = slot_ids[None, :] < send_counts[:, part_index][:, None]
            halo_rows = jnp.where(live_mask[:, :, None], layer_table[source_rows], jnp.zeros((), jnp.bfloat16))
            halo_rows = halo_rows.reshape(N_DOM * CAP, F)
            own_rows = lax.dynamic_slice_in_dim(current, (part_index * NODES_DEV).astype(jnp.int32), NODES_DEV, 0)
            combined = jnp.concatenate([own_rows, halo_rows], axis=0).reshape(-1, TILE, F)
            columns = lax.dynamic_slice_in_dim(tile_columns, (part_index * local_tiles).astype(jnp.int32), local_tiles, 0)
            values = lax.dynamic_slice_in_dim(tile_values, (part_index * local_tiles).astype(jnp.int32), local_tiles, 0)
            picked = combined[columns]
            summed = jnp.einsum('rkab,rkbf->raf', values.astype(jnp.float32), picked.astype(jnp.float32))
            return summed.reshape(NODES_DEV, F)

        aggregated = lax.map(one_part, jnp.arange(N_DOM, dtype=jnp.int32)).reshape(NODES, F)
        blended = ((1.0 - ALPHA) * aggregated + ALPHA * initial.astype(jnp.float32)).astype(jnp.bfloat16)
        blended = lax.optimization_barrier(blended)
        product = jnp.dot(blended, layer_weights[layer_index], preferred_element_type=jnp.float32)
        fresh = jnp.maximum((1.0 - beta_layer) * blended.astype(jnp.float32) + beta_layer * product, 0.0)
        pushed.append(current)
        current = fresh.astype(jnp.bfloat16)
    return jnp.stack(pushed), current
```

```python
import functools
import math

import jax
import jax.numpy as jnp
from jax import lax
from jax.experimental import pallas as pl
from jax.experimental.pallas import tpu as pltpu
from jax.sharding import PartitionSpec as P

ALPHA = 0.1
LAMBDA_DECAY = 0.5
CORES = 2
GROUP = 4
GATHER_LAG = 3
OWN_TILES = 2
MESH = pl.DeviceIdType.MESH
NT = (((1,), (1,)), ((), ()))


def gather_order(doms):
    quarter = doms // 4
    places = []
    for place in range(quarter):
        places.append(("I", place))
        places += [("N", index) for index in (2 * place, 2 * place + 1) if index < doms // 2 - 1]
        places.append(("O", place))
    return places


def kernel(
    doms, feats, layers, tile, columns_ref, counts_ref, rows_ref, history_hbm, features_hbm,
    w_ref, weights_ref, values_hbm, pushed_hbm, final_hbm, *scratch
):
    halos = scratch[:layers]
    (history, features, w_all, weights_t, last_w, values, outgoing, initial, ping, pong, partial, final,
     load_sem, w_send, w_recv, z_send, z_recv, y_send, y_recv, c_send, c_recv, out_sem,
     final_sem) = scratch[layers:]
    width = w_ref.shape[0]
    nodes = history.shape[1]
    cap = rows_ref.shape[1]
    row_tiles, per_row = values.shape[0], values.shape[1]
    hidden = width * feats
    chips = feats // CORES
    dom = lax.axis_index("dom")
    feat = lax.axis_index("feat")
    chip, core = feat // CORES, feat % CORES
    sibling = chip * CORES + (1 - core)

    loads = [
        pltpu.make_async_copy(history_hbm, history, load_sem.at[0]),
        pltpu.make_async_copy(features_hbm, features, load_sem.at[1]),
        pltpu.make_async_copy(values_hbm, values, load_sem.at[2]),
    ]
    for load in loads:
        load.start()

    barrier = pltpu.get_barrier_semaphore()
    for step in range(1, doms):
        pl.semaphore_signal(
            barrier, inc=1, device_id={"dom": lax.rem(dom + step, doms)}, device_id_type=MESH
        )
    for step in range(1, feats):
        pl.semaphore_signal(
            barrier, inc=1, device_id={"feat": lax.rem(feat + step, feats)}, device_id_type=MESH
        )

    def slice_rows(index):
        return pl.ds(pl.multiple_of(index * width, width), width)

    blocks = cap // tile

    half, quarter = doms // 2, doms // 4
    inside = lax.rem(dom // quarter + 1, 4) // 2
    near = [(flips, 0) for flips in range(1, half)]
    outer = [(half + quarter + index, -quarter) for index in range(quarter)]
    inner = [(half + index, quarter) for index in range(quarter)]
    groups = {"N": near, "O": outer, "I": inner}

    def chosen(table, index):
        if isinstance(index, int):
            base, slope = table[index]
            return base + slope * inside
        value = 0
        for place, (base, slope) in enumerate(table):
            value = value + jnp.where(index == place, base + slope * inside, 0)
        return value

    def partner(flips):
        dest, bit = dom, 1
        while bit < doms:
            dest = dest + lax.rem(flips // bit, 2) * (bit - 2 * bit * lax.rem(dom // bit, 2))
            bit *= 2
        return dest

    def block_tiles(source):
        return pl.ds(source * blocks, blocks)

    def w_copy(step):
        return pltpu.make_async_remote_copy(
            src_ref=w_ref,
            dst_ref=w_all.at[slice_rows(feat)],
            send_sem=w_send.at[step],
            recv_sem=w_recv.at[step],
            device_id={"feat": lax.rem(feat + step, feats)},
            device_id_type=MESH,
        )

    def z_copy(level, flips):
        return pltpu.make_async_remote_copy(
            src_ref=outgoing.at[flips, :, pl.ds(level * width, width)],
            dst_ref=halos[level].at[block_tiles(dom), slice_rows(feat)],
            send_sem=z_send.at[level, flips],
            recv_sem=z_recv.at[level, flips],
            device_id={"dom": partner(flips)},
            device_id_type=MESH,
        )

    def y_copy(level, flips, hop):
        block = halos[level].at[block_tiles(partner(flips)), slice_rows(feat)]
        return pltpu.make_async_remote_copy(
            src_ref=block,
            dst_ref=block,
            send_sem=y_send.at[level, flips, hop],
            recv_sem=y_recv.at[level, flips, hop],
            device_id={"feat": lax.rem(chip + hop, chips) * CORES + core},
            device_id_type=MESH,
        )

    def c_copy(level, flips, hop):
        owner = lax.rem(chip + chips - hop, chips) * CORES + core
        block = halos[level].at[block_tiles(partner(flips)), slice_rows(owner)]
        return pltpu.make_async_remote_copy(
            src_ref=block,
            dst_ref=block,
            send_sem=c_send.at[level, flips, hop],
            recv_sem=c_recv.at[level, flips, hop],
            device_id={"feat": sibling},
            device_id_type=MESH,
        )

    def gather(flips):
        dest = partner(flips)
        part = min(cap, 256)
        for begin in range(0, cap, part):
            slots = begin + lax.broadcasted_iota(jnp.int32, (1, part), 1)
            rows = rows_ref[pl.ds(dest, 1), pl.ds(begin, part)]
            rows = jnp.where(slots < counts_ref[0, dest], rows, -1)
            nodes_iota = lax.broadcasted_iota(jnp.int32, (nodes, part), 0)
            onehot = jnp.where(nodes_iota == rows, 1.0, 0.0).astype(jnp.bfloat16)
            picked = jnp.dot(history[...], onehot, preferred_element_type=jnp.float32)
            picked = picked.astype(jnp.bfloat16)
            for offset in range(0, part, tile):
                outgoing[flips, (begin + offset) // tile] = picked[:, offset : offset + tile]

    def arrive(level, flips):
        z_copy(level, flips).wait_recv()
        for hop in range(1, chips):
            y_copy(level, flips, hop).start()
        c_copy(level, flips, 0).start()

    def relay(level, flips):
        for hop in range(1, chips):
            y_copy(level, flips, hop).wait_recv()
            c_copy(level, flips, hop).start()

    def settle(level):
        def step(flips, carry):
            for hop in range(chips):
                c_copy(level, flips, hop).wait_recv()
            return carry

        lax.fori_loop(1, doms, step, 0)

    group = GROUP

    def initial_group(index):
        span = group * tile
        part = pl.ds(pl.multiple_of(index * span, span), span)
        product = lax.dot_general(
            w_all[...], features[part, :], NT, preferred_element_type=jnp.float32
        )
        product = jnp.maximum(product, 0.0).astype(jnp.bfloat16)
        for offset in range(group):
            initial[index * group + offset] = product[:, offset * tile : (offset + 1) * tile]

    def turn_group(index):
        for offset in range(group):
            row = index * group + offset
            for k in range(per_row):
                values[row, k] = values[row, k].T

    def push(level, buffer):
        return pltpu.make_async_copy(
            buffer.at[:, slice_rows(feat)], pushed_hbm.at[level], out_sem.at[level]
        )

    states = [initial] + [ping if index % 2 == 0 else pong for index in range(layers - 1)]

    def summed(row, first, last, current, halo):
        picked = []
        for k in range(first, last):
            column = columns_ref[k, row]
            if k < OWN_TILES:
                picked.append(current[column])
            else:
                picked.append(halo[jnp.maximum(column - row_tiles, 0)])
        return jnp.dot(
            jnp.concatenate(picked, axis=1),
            values[row, first:last].reshape((last - first) * tile, tile),
            preferred_element_type=jnp.float32,
        )

    def layer_group(layer, index):
        beta = math.log(LAMBDA_DECAY / (layer + 1) + 1.0)
        current, following, halo = states[layer], states[layer + 1], halos[layer]
        first = index * group
        pieces = []
        for offset in range(group):
            row = first + offset
            total = summed(row, 0, per_row, current, halo)
            start = initial[row].astype(jnp.float32)
            pieces.append(((1.0 - ALPHA) * total + ALPHA * start).astype(jnp.bfloat16))
        blended = jnp.concatenate(pieces, axis=1)
        product = jnp.dot(weights_t[layer], blended, preferred_element_type=jnp.float32)
        fresh = jnp.maximum((1.0 - beta) * blended.astype(jnp.float32) + beta * product, 0.0)
        fresh = fresh.astype(jnp.bfloat16)
        for offset in range(group):
            following[first + offset] = fresh[:, offset * tile : (offset + 1) * tile]

    last = layers - 1

    def own_group(index):
        for offset in range(group):
            row = index * group + offset
            total = summed(row, 0, OWN_TILES, states[last], None)
            start = initial[row].astype(jnp.float32)
            partial[row] = (1.0 - ALPHA) * total + ALPHA * start

    def final_copy(index):
        part = pl.ds(index * group, group)
        return pltpu.make_async_copy(final.at[part], final_hbm.at[part], final_sem.at[index])

    def last_group(index):
        beta = math.log(LAMBDA_DECAY / layers + 1.0)
        first = index * group
        pieces = []
        for offset in range(group):
            row = first + offset
            total = summed(row, OWN_TILES, per_row, None, halos[last])
            pieces.append((partial[row] + (1.0 - ALPHA) * total).astype(jnp.bfloat16))
        blended = jnp.concatenate(pieces, axis=1)
        product = jnp.dot(last_w[...], blended, preferred_element_type=jnp.float32)
        fresh = jnp.maximum((1.0 - beta) * product[:width] + beta * product[width:], 0.0)
        fresh = fresh.astype(jnp.bfloat16)
        for offset in range(group):
            final[first + offset] = fresh[:, offset * tile : (offset + 1) * tile]
        final_copy(index).start()

    count = row_tiles // group

    def loop(begin, end, body):
        def step(index, carry):
            body(index)
            return carry

        lax.fori_loop(begin, end, step, 0)

    order = [groups[kind][place] for kind, place in gather_order(doms)]
    loads[0].wait()
    gather(chosen(order, 0))
    pl.semaphore_wait(barrier, doms + feats - 2)
    z_copy(0, chosen(order, 0)).start()
    for step in range(1, feats):
        w_copy(step).start()

    def gather_step(index):
        flips = chosen(order, index)
        gather(flips)
        z_copy(0, flips).start()

    def gather_arrive(index):
        gather_step(index)
        arrive(0, chosen(order, index - GATHER_LAG))

    loop(1, GATHER_LAG, gather_step)
    loop(GATHER_LAG, doms - 1, gather_arrive)
    for level in range(1, layers):
        loop(0, doms - 1, lambda index, level=level: z_copy(level, chosen(order, index)).start())

    for level in range(layers):
        halos[level][block_tiles(dom)] = jnp.zeros((blocks, hidden, tile), jnp.bfloat16)
        weights_t[level] = weights_ref[level].astype(jnp.float32).T.astype(jnp.bfloat16)
    rows_iota = lax.broadcasted_iota(jnp.int32, (width, hidden), 0)
    columns_iota = lax.broadcasted_iota(jnp.int32, (width, hidden), 1)
    last_w[:width] = jnp.where(rows_iota + feat * width == columns_iota, 1.0, 0.0).astype(jnp.bfloat16)
    last_w[width:] = weights_t[last, slice_rows(feat)]
    loop(doms - 1 - GATHER_LAG, doms - 1, lambda index: arrive(0, chosen(order, index)))

    w_all[slice_rows(feat), :] = w_ref[...]
    for step in range(1, feats):
        w_copy(step).wait_recv()
    loads[1].wait()

    works = {
        "initial": initial_group,
        "turn": turn_group,
        "own": own_group,
        "last": last_group,
    }
    for layer in range(last):
        works["layer" + str(layer)] = functools.partial(layer_group, layer)
    done = {name: 0 for name in works}

    def run(name, pieces):
        begin = done[name]
        done[name] = end = min(begin + pieces, count)
        loop(begin, end, works[name])

    def arrivals(code, name=None, each=0):
        table, level = groups[code[0]], int(code[1])
        if name is None or each == 0:
            loop(0, len(table), lambda index: arrive(level, chosen(table, index)))
            return
        begin = done[name]
        fused = min(len(table), (count - begin) // each)
        done[name] = begin + fused * each

        def body(index):
            arrive(level, chosen(table, index))
            for extra in range(each):
                works[name](begin + index * each + extra)

        loop(0, fused, body)
        loop(fused, len(table), lambda index: arrive(level, chosen(table, index)))

    def relays(codes):
        for code in codes.split():
            if code[0] == "A":
                loop(0, doms - 1, lambda index: relay(int(code[1]), chosen(order, index)))
            else:
                table = groups[code[0]]
                loop(0, len(table), lambda index: relay(int(code[1]), chosen(table, index)))

    arrivals("N1", "initial", 2)
    run("initial", count)
    push(0, initial).start()
    loads[2].wait()
    arrivals("O1", "turn", 2)
    run("turn", count)
    relays("A0")
    settle(0)
    for code in ("N2", "N3", "O2"):
        arrivals(code, "layer0", 1)
    run("layer0", count)
    push(1, states[1]).start()
    arrivals("I1")
    relays("N1 O1 I1")
    settle(1)
    arrivals("O3", "layer1", 1)
    run("layer1", count)
    push(2, states[2]).start()
    arrivals("I2")
    relays("N2 O2 I2")
    settle(2)
    push(1, states[1]).wait()
    run("layer2", 4)
    arrivals("I3", "layer2", 1)
    run("layer2", count)
    push(3, states[3]).start()
    run("own", 4)
    relays("N3 O3")
    run("own", count)
    relays("I3")
    settle(3)
    run("last", count)

    for step in range(1, feats):
        w_copy(step).wait_send()
    for level in range(layers):

        def drain(flips, level=level):
            z_copy(level, flips).wait_send()
            for hop in range(chips):
                c_copy(level, flips, hop).wait_send()
            for hop in range(1, chips):
                y_copy(level, flips, hop).wait_send()

        loop(1, doms, drain)
    loop(0, count, lambda index: final_copy(index).wait())
    for level in (0, 2, 3):
        push(level, states[level]).wait()


def on_device(doms, feats, features, w_input, layer_weights, history, tile_values, tile_columns, send_rows, send_counts):
    layers, nodes, width = history.shape
    row_tiles, per_row, tile, _ = tile_values.shape
    cap = send_rows.shape[2]
    hidden = width * feats
    chips = feats // CORES
    any_spec = pl.BlockSpec(memory_space=pl.ANY)
    vmem = pl.BlockSpec(memory_space=pltpu.VMEM)
    smem = pl.BlockSpec(memory_space=pltpu.SMEM)
    bf16 = jnp.bfloat16
    dma = pltpu.SemaphoreType.DMA
    pushed, final = pl.pallas_call(
        functools.partial(kernel, doms, feats, layers, tile),
        out_shape=(
            jax.ShapeDtypeStruct((layers, row_tiles, width, tile), bf16),
            jax.ShapeDtypeStruct((row_tiles, width, tile), bf16),
        ),
        in_specs=[smem, smem, vmem, any_spec, any_spec, vmem, vmem, any_spec],
        out_specs=(any_spec, any_spec),
        scratch_shapes=[pltpu.VMEM((doms * cap // tile, hidden, tile), bf16) for _ in range(layers)] + [
            pltpu.VMEM((layers * width, nodes), bf16),
            pltpu.VMEM(features.shape, bf16),
            pltpu.VMEM((hidden, features.shape[1]), bf16),
            pltpu.VMEM((layers, hidden, hidden), bf16),
            pltpu.VMEM((2 * width, hidden), bf16),
            pltpu.VMEM(tile_values.shape, bf16),
            pltpu.VMEM((doms, cap // tile, layers * width, tile), bf16),
            pltpu.VMEM((row_tiles, hidden, tile), bf16),
            pltpu.VMEM((row_tiles, hidden, tile), bf16),
            pltpu.VMEM((row_tiles, hidden, tile), bf16),
            pltpu.VMEM((row_tiles, hidden, tile), jnp.float32),
            pltpu.VMEM((row_tiles, width, tile), bf16),
            dma((3,)),
            dma((feats,)),
            dma((feats,)),
            dma((layers, doms)),
            dma((layers, doms)),
            dma((layers, doms, chips)),
            dma((layers, doms, chips)),
            dma((layers, doms, chips)),
            dma((layers, doms, chips)),
            dma((layers,)),
            dma((row_tiles // GROUP,)),
        ],
        compiler_params=pltpu.CompilerParams(
            collective_id=0, has_side_effects=True, vmem_limit_bytes=67043328
        ),
    )(
        tile_columns.T,
        send_counts,
        send_rows[0],
        jnp.swapaxes(history, 1, 2).reshape(layers * width, nodes),
        features,
        w_input.T,
        layer_weights,
        tile_values,
    )
    pushed = jnp.transpose(pushed, (0, 1, 3, 2)).reshape(layers, nodes, width)
    return pushed, jnp.transpose(final, (0, 2, 1)).reshape(nodes, width)


def solution(mesh):
    placed = (
        P("dom", None),
        P(None, "feat"),
        P(),
        P(None, "dom", "feat"),
        P("dom", None, None, None),
        P("dom", None),
        P("dom", None, None),
        P("dom", None),
    )
    return jax.shard_map(
        functools.partial(on_device, mesh.shape["dom"], mesh.shape["feat"]),
        mesh=mesh,
        in_specs=placed,
        out_specs=(P(None, "dom", "feat"), P("dom", "feat")),
        check_vma=False,
    )
```

```python
import functools
import math

import jax
import jax.numpy as jnp
from jax import lax
from jax.experimental import pallas as pl
from jax.experimental.pallas import tpu as pltpu
from jax.sharding import PartitionSpec as P

ALPHA = 0.1
LAMBDA_DECAY = 0.5
CORES = 2
GROUP = 8
ORDER = ("O0", "I0", "O1", "I1", "X0", "N0", "N1")
ARRIVALS = (
    ("G0", "H0", "N0", "X0", "N1", "N2", "O1", "X1", "I1")
    + ("N3", "X2", "O2", "I2", "X3", "O3", "I3")
)
EARLY = 6
LAG = 4
PACE_KIND = "O"
SLACK = 1
OWN_TILES = 2
MESH = pl.DeviceIdType.MESH
NT = (((1,), (1,)), ((), ()))


def kernel(
    doms, feats, layers, tile, columns_ref, counts_ref, rows_hbm, history_hbm, features_hbm,
    w_hbm, weights_hbm, values_hbm, pushed_ref, final_ref, *scratch
):
    halos = scratch[:layers]
    (rows_ref, w_ref, weights_ref, history, features, w_all, weights_t, last_w, values, outgoing, initial, ping, pong, partial,
     load_sem, w_send, w_recv, z_send, z_recv, y_send, y_recv, c_send, c_recv) = scratch[layers:]
    width = w_ref.shape[0]
    nodes = history.shape[1]
    cap = rows_ref.shape[1]
    row_tiles, per_row = values.shape[0], values.shape[1]
    hidden = width * feats
    chips = feats // CORES
    dom = lax.axis_index("dom")
    feat = lax.axis_index("feat")
    chip, core = feat // CORES, feat % CORES
    sibling = chip * CORES + (1 - core)

    half, quarter = doms // 2, doms // 4
    inside = lax.rem(dom // quarter + 1, 4) // 2
    near = [(flips, 0) for flips in range(2, half)]
    outer = [(half + quarter + index, -quarter) for index in range(quarter)]
    inner = [(half + index, quarter) for index in range(quarter)]
    groups = {"X": [(1, 0)], "N": near, "O": outer, "I": inner}

    def chosen(table, index):
        if isinstance(index, int):
            base, slope = table[index]
            return base + slope * inside
        value = 0
        for place, (base, slope) in enumerate(table):
            value = value + jnp.where(index == place, base + slope * inside, 0)
        return value

    def partner(flips):
        dest, bit = dom, 1
        while bit < doms:
            dest = dest + lax.rem(flips // bit, 2) * (bit - 2 * bit * lax.rem(dom // bit, 2))
            bit *= 2
        return dest

    barrier = pltpu.get_barrier_semaphore()
    for step in range(1, doms):
        pl.semaphore_signal(
            barrier, inc=1, device_id={"dom": lax.rem(dom + step, doms)}, device_id_type=MESH
        )
    for step in range(1, feats):
        pl.semaphore_signal(
            barrier, inc=1, device_id={"feat": lax.rem(feat + step, feats)}, device_id_type=MESH
        )
    for hop in range(1, chips):
        across = {"dom": partner(1), "feat": lax.rem(chip + hop, chips) * CORES + core}
        pl.semaphore_signal(barrier, inc=1, device_id=across, device_id_type=MESH)

    rows_load = pltpu.make_async_copy(rows_hbm, rows_ref, load_sem.at[5])
    loads = [
        pltpu.make_async_copy(history_hbm, history, load_sem.at[0]),
        pltpu.make_async_copy(features_hbm, features, load_sem.at[1]),
        pltpu.make_async_copy(values_hbm, values, load_sem.at[2]),
        pltpu.make_async_copy(w_hbm, w_ref, load_sem.at[3]),
        pltpu.make_async_copy(weights_hbm, weights_ref, load_sem.at[4]),
    ]
    for load in (loads[0], rows_load, *loads[1:]):
        load.start()

    def slice_rows(index):
        return pl.ds(pl.multiple_of(index * width, width), width)

    blocks = cap // tile

    def block_tiles(source):
        return pl.ds(source * blocks, blocks)

    def w_copy(step):
        return pltpu.make_async_remote_copy(
            src_ref=w_ref,
            dst_ref=w_all.at[slice_rows(feat)],
            send_sem=w_send.at[step],
            recv_sem=w_recv.at[step],
            device_id={"feat": lax.rem(feat + step, feats)},
            device_id_type=MESH,
        )

    def z_copy(level, flips):
        return pltpu.make_async_remote_copy(
            src_ref=outgoing.at[flips, :, pl.ds(level * width, width)],
            dst_ref=halos[level].at[block_tiles(dom), slice_rows(feat)],
            send_sem=z_send.at[0],
            recv_sem=z_recv.at[level, flips],
            device_id={"dom": partner(flips)},
            device_id_type=MESH,
        )

    def y_copy(level, flips, hop):
        block = halos[level].at[block_tiles(partner(flips)), slice_rows(feat)]
        return pltpu.make_async_remote_copy(
            src_ref=block,
            dst_ref=block,
            send_sem=y_send.at[hop],
            recv_sem=y_recv.at[level, flips, hop],
            device_id={"feat": lax.rem(chip + hop, chips) * CORES + core},
            device_id_type=MESH,
        )

    def x_copy(level, hop):
        return pltpu.make_async_remote_copy(
            src_ref=outgoing.at[1, :, pl.ds(level * width, width)],
            dst_ref=halos[level].at[block_tiles(dom), slice_rows(feat)],
            send_sem=y_send.at[hop],
            recv_sem=y_recv.at[level, 1, hop],
            device_id={"dom": partner(1), "feat": lax.rem(chip + hop, chips) * CORES + core},
            device_id_type=MESH,
        )

    def x_send(level):
        z_copy(level, 1).start()
        for hop in range(1, chips):
            x_copy(level, hop).start()

    def c_copy(level, flips, hop):
        owner = lax.rem(chip + chips - hop, chips) * CORES + core
        block = halos[level].at[block_tiles(partner(flips)), slice_rows(owner)]
        return pltpu.make_async_remote_copy(
            src_ref=block,
            dst_ref=block,
            send_sem=c_send.at[hop],
            recv_sem=c_recv.at[level],
            device_id={"feat": sibling},
            device_id_type=MESH,
        )

    def gather(flips):
        dest = partner(flips)
        part = min(cap, 256)
        for begin in range(0, cap, part):
            slots = begin + lax.broadcasted_iota(jnp.int32, (1, part), 1)
            rows = rows_ref[pl.ds(dest, 1), pl.ds(begin, part)]
            rows = jnp.where(slots < counts_ref[0, dest], rows, -1)
            nodes_iota = lax.broadcasted_iota(jnp.int32, (nodes, part), 0)
            onehot = jnp.where(nodes_iota == rows, 1.0, 0.0).astype(jnp.bfloat16)
            picked = jnp.dot(history[...], onehot, preferred_element_type=jnp.float32)
            picked = picked.astype(jnp.bfloat16)
            for offset in range(0, part, tile):
                outgoing[flips, (begin + offset) // tile] = picked[:, offset : offset + tile]

    def arrive(level, kind, flips, index):
        z_copy(level, flips).wait_recv()
        if kind == "N" and level + 2 < layers:
            z_copy(level + 2, flips).start()
        if kind == PACE_KIND and level + 1 < layers:

            @pl.when(inside == 0)
            def _():
                z_copy(level + 1, chosen(outer, index)).start()
                z_copy(level + 1, chosen(inner, index)).start()

        if kind != "X":
            for hop in range(1, chips):
                y_copy(level, flips, hop).start()
        elif level + 2 < layers:
            x_send(level + 2)
        c_copy(level, flips, 0).start()

    def relay(level, flips):
        for hop in range(1, chips):
            y_copy(level, flips, hop).wait_recv()
            c_copy(level, flips, hop).start()

    def settle(level):
        span = halos[level].at[pl.ds(0, (doms - 1) * chips * blocks // feats)]
        pltpu.make_async_remote_copy(
            src_ref=span,
            dst_ref=span,
            send_sem=c_send.at[0],
            recv_sem=c_recv.at[level],
            device_id={"feat": sibling},
            device_id_type=MESH,
        ).wait_recv()

    def drain(sem):
        span = outgoing.at[pl.ds(1, doms - 1)]
        pltpu.make_async_remote_copy(
            src_ref=span,
            dst_ref=span,
            send_sem=sem,
            recv_sem=c_recv.at[0],
            device_id={"feat": sibling},
            device_id_type=MESH,
        ).wait_send()

    group = GROUP

    def initial_group(index):
        span = group * tile
        part = pl.ds(pl.multiple_of(index * span, span), span)
        product = lax.dot_general(
            w_all[...], features[part, :], NT, preferred_element_type=jnp.float32
        )
        product = jnp.maximum(product, 0.0).astype(jnp.bfloat16)
        for offset in range(group):
            initial[index * group + offset] = product[:, offset * tile : (offset + 1) * tile]

    states = [initial] + [ping if index % 2 == 0 else pong for index in range(layers - 1)]

    def summed(row, first, last, current, halo):
        picked = []
        for k in range(first, last):
            column = columns_ref[k, row]
            if k < OWN_TILES:
                picked.append(current[column])
            else:
                picked.append(halo[jnp.maximum(column - row_tiles, 0)])
        return lax.dot_general(
            jnp.concatenate(picked, axis=1),
            jnp.concatenate([values[row, k] for k in range(first, last)], axis=1),
            NT,
            preferred_element_type=jnp.float32,
        )

    last = layers - 1

    def own_group(layer, index):
        for offset in range(group):
            row = index * group + offset
            total = summed(row, 0, OWN_TILES, states[layer], None)
            start = initial[row].astype(jnp.float32)
            partial[row] = (1.0 - ALPHA) * total + ALPHA * start
            columns = pl.ds(pl.multiple_of(row * tile, tile), tile)
            pushed_ref[layer, :, columns] = states[layer][row, slice_rows(feat), :]

    def blended_group(layer, index):
        pieces = []
        for offset in range(group):
            row = index * group + offset
            total = summed(row, OWN_TILES, per_row, None, halos[layer])
            pieces.append((partial[row] + (1.0 - ALPHA) * total).astype(jnp.bfloat16))
        return jnp.concatenate(pieces, axis=1)

    def layer_group(layer, index):
        beta = math.log(LAMBDA_DECAY / (layer + 1) + 1.0)
        following = states[layer + 1]
        blended = blended_group(layer, index)
        product = jnp.dot(weights_t[layer], blended, preferred_element_type=jnp.float32)
        fresh = jnp.maximum((1.0 - beta) * blended.astype(jnp.float32) + beta * product, 0.0)
        fresh = fresh.astype(jnp.bfloat16)
        for offset in range(group):
            following[index * group + offset] = fresh[:, offset * tile : (offset + 1) * tile]

    def last_group(index):
        beta = math.log(LAMBDA_DECAY / layers + 1.0)
        blended = blended_group(last, index)
        product = jnp.dot(last_w[...], blended, preferred_element_type=jnp.float32)
        fresh = jnp.maximum((1.0 - beta) * product[:width] + beta * product[width:], 0.0)
        fresh = fresh.astype(jnp.bfloat16)
        span = group * tile
        final_ref[:, pl.ds(pl.multiple_of(index * span, span), span)] = fresh

    count = row_tiles // group

    def loop(begin, end, body):
        def step(index, carry):
            body(index)
            return carry

        lax.fori_loop(begin, end, step, 0)

    order = [groups[code[0]][int(code[1:])] for code in ORDER]
    rows_load.wait()
    loads[0].wait()
    gather(chosen(order, 0))
    pl.semaphore_wait(barrier, doms + feats + chips - 3)
    if order[0] == (1, 0):
        x_send(0)
        x_send(1)
    else:
        z_copy(0, chosen(order, 0)).start()
    loads[3].wait()
    for step in range(1, feats):
        w_copy(step).start()

    def gather_step(index):
        flips = chosen(order, index)
        gather(flips)
        z_copy(0, flips).start()

    far = [entry for pair in zip(outer, inner) for entry in pair]
    arriving = []
    for code in ARRIVALS:
        level = int(code[1])
        if code[0] in "GH":
            part = far[: half // 2] if code[0] == "G" else far[half // 2 :]
            arriving += [(level, entry, "O" if entry in outer else "I") for entry in part]
        else:
            arriving += [(level, entry, code[0]) for entry in groups[code[0]]]
    early = doms - 1 - EARLY

    cross = order.index((1, 0))

    def gather_span(begin, end):
        if begin <= cross < end:
            loop(begin, cross, gather_step)
            gather(1)
            x_send(0)
            x_send(1)
            begin = cross + 1
        loop(begin, end, gather_step)

    gather_span(1, EARLY)
    for index in range(early):
        gather_span(EARLY + index, EARLY + index + 1)
        level, entry, kind = arriving[index]
        arrive(level, kind, chosen([entry], 0), groups[kind].index(entry))
    loop(0, len(near), lambda index: z_copy(1, chosen(near, index)).start())

    @pl.when(inside == 1)
    def _():
        for level in range(1, layers):
            loop(0, quarter, lambda index: z_copy(level, chosen(outer, index)).start())
            loop(0, quarter, lambda index: z_copy(level, chosen(inner, index)).start())

    loads[4].wait()
    for level in range(layers):
        halos[level][block_tiles(dom)] = jnp.zeros((blocks, hidden, tile), jnp.bfloat16)
        weights_t[level] = weights_ref[level].astype(jnp.float32).T.astype(jnp.bfloat16)
    rows_iota = lax.broadcasted_iota(jnp.int32, (width, hidden), 0)
    columns_iota = lax.broadcasted_iota(jnp.int32, (width, hidden), 1)
    last_w[:width] = jnp.where(rows_iota + feat * width == columns_iota, 1.0, 0.0).astype(jnp.bfloat16)
    last_w[width:] = weights_t[last, slice_rows(feat)]

    w_all[slice_rows(feat), :] = w_ref[...]
    for step in range(1, feats):
        w_copy(step).wait_recv()
    loads[1].wait()

    works = {"initial": initial_group}
    for layer in range(last):
        works["own" + str(layer)] = functools.partial(own_group, layer)
        works["layer" + str(layer)] = functools.partial(layer_group, layer)
    works["own" + str(last)] = functools.partial(own_group, last)
    works["last"] = last_group
    done = {name: 0 for name in works}

    def run(name, pieces):
        begin = done[name]
        done[name] = end = min(begin + pieces, count)
        loop(begin, end, works[name])

    final_step = len(arriving) + LAG
    covered = [
        max(place for place, entry in enumerate(arriving) if entry[0] == layer) + LAG + 1
        for layer in range(layers)
    ]

    def before(name):
        if name == "own0":
            loads[2].wait()
        if name.startswith("layer"):
            settle(int(name[5:]))
        if name == "last":
            settle(last)

    pieces = [("initial", 0)] * count
    for layer in range(last):
        pieces += [("own" + str(layer), 0)] * count
        pieces += [("layer" + str(layer), covered[layer] + SLACK)] * count
    pieces += [("own" + str(last), 0)] * count
    plan = []
    for step in range(early, final_step):
        piece = pieces.pop(0)[0] if pieces and pieces[0][1] <= step else None
        plan.append(
            (
                arriving[step] if step < len(arriving) else None,
                arriving[step - LAG] if step >= LAG else None,
                piece,
            )
        )

    def like(entry):
        arrived, relayed, piece = entry
        return (arrived and (arrived[0], arrived[2]), relayed and relayed[0], piece)

    while plan:
        length = 1
        while length < len(plan) and like(plan[length]) == like(plan[0]):
            length += 1
        part, plan = plan[:length], plan[length:]
        arrived, relayed, piece = part[0]
        begin = 0
        if piece:
            begin = done[piece]
            done[piece] += length
            if begin == 0:
                before(piece)

        def body(index, part=part, arrived=arrived, relayed=relayed, piece=piece, begin=begin):
            if arrived:
                table = [entry[0][1] for entry in part]
                place = groups[arrived[2]].index(table[0]) + index
                arrive(arrived[0], arrived[2], chosen(table, index), place)
            if relayed:
                relay(relayed[0], chosen([entry[1][1] for entry in part], index))
            if piece:
                works[piece](begin + index)

        loop(0, length, body)
    for name in [*works]:
        if done[name] < count:
            if done[name] == 0:
                before(name)
            run(name, count)

    for step in range(1, feats):
        w_copy(step).wait_send()
    drain(z_send.at[0])
    for hop in range(1, chips):
        drain(y_send.at[hop])
    for hop in range(chips):
        drain(c_send.at[hop])


def on_device(doms, feats, features, w_input, layer_weights, history, tile_values, tile_columns, send_rows, send_counts):
    layers, nodes, width = history.shape
    row_tiles, per_row, tile, _ = tile_values.shape
    cap = send_rows.shape[2]
    hidden = width * feats
    chips = feats // CORES
    any_spec = pl.BlockSpec(memory_space=pl.ANY)
    smem = pl.BlockSpec(memory_space=pltpu.SMEM)
    bf16 = jnp.bfloat16
    dma = pltpu.SemaphoreType.DMA
    pushed, final = pl.pallas_call(
        functools.partial(kernel, doms, feats, layers, tile),
        out_shape=(
            pltpu.VMEM((layers, width, nodes), bf16),
            pltpu.VMEM((width, nodes), bf16),
        ),
        in_specs=[smem, smem] + [any_spec] * 6,
        out_specs=(pl.BlockSpec(memory_space=pltpu.VMEM), pl.BlockSpec(memory_space=pltpu.VMEM)),
        scratch_shapes=[pltpu.VMEM((doms * cap // tile, hidden, tile), bf16) for _ in range(layers)] + [
            pltpu.VMEM(send_rows.shape[1:], jnp.int32),
            pltpu.VMEM((width, features.shape[1]), bf16),
            pltpu.VMEM(layer_weights.shape, bf16),
            pltpu.VMEM((layers * width, nodes), bf16),
            pltpu.VMEM(features.shape, bf16),
            pltpu.VMEM((hidden, features.shape[1]), bf16),
            pltpu.VMEM((layers, hidden, hidden), bf16),
            pltpu.VMEM((2 * width, hidden), bf16),
            pltpu.VMEM(tile_values.shape, bf16),
            pltpu.VMEM((doms, cap // tile, layers * width, tile), bf16),
            pltpu.VMEM((row_tiles, hidden, tile), bf16),
            pltpu.VMEM((row_tiles, hidden, tile), bf16),
            pltpu.VMEM((row_tiles, hidden, tile), bf16),
            pltpu.VMEM((row_tiles, hidden, tile), jnp.float32),
            dma((6,)),
            dma((feats,)),
            dma((feats,)),
            dma((1,)),
            dma((layers, doms)),
            dma((chips,)),
            dma((layers, doms, chips)),
            dma((chips,)),
            dma((layers,)),
        ],
        compiler_params=pltpu.CompilerParams(
            collective_id=0, has_side_effects=True, vmem_limit_bytes=67043328 - 2 * (layers + 1) * width * nodes
        ),
    )(
        tile_columns.T,
        send_counts,
        send_rows[0],
        jnp.swapaxes(history, 1, 2).reshape(layers * width, nodes),
        features,
        w_input.T,
        layer_weights,
        tile_values,
    )
    return jnp.swapaxes(pushed, 1, 2), final.T


def solution(mesh):
    placed = (
        P("dom", None),
        P(None, "feat"),
        P(),
        P(None, "dom", "feat"),
        P("dom", None, None, None),
        P("dom", None),
        P("dom", None, None),
        P("dom", None),
    )
    return jax.shard_map(
        functools.partial(on_device, mesh.shape["dom"], mesh.shape["feat"]),
        mesh=mesh,
        in_specs=placed,
        out_specs=(P(None, "dom", "feat"), P("dom", "feat")),
        check_vma=False,
    )
```

```python
import functools
import math

import jax
import jax.numpy as jnp
from jax import lax
from jax.experimental import pallas as pl
from jax.experimental.pallas import tpu as pltpu
from jax.sharding import PartitionSpec as P

ALPHA = 0.1
LAMBDA_DECAY = 0.5
CORES = 2
GROUP = 8
ORDER = ("O0", "I0", "O1", "I1", "X0", "N0", "N1")
ARRIVALS = (
    ("G0", "H0", "N0", "X0", "N1", "N2", "O1", "X1", "I1")
    + ("N3", "X2", "O2", "I2", "X3", "O3", "I3")
)
EARLY = 6
LAG = 5
PACE_KINDS = ("O", "O", "O")
WIDE = 2
SLACK = 0
OWN_TILES = 2
MESH = pl.DeviceIdType.MESH
NT = (((1,), (1,)), ((), ()))


def kernel(
    doms, feats, layers, tile, columns_ref, counts_ref, rows_hbm, history_hbm, features_hbm,
    w_hbm, weights_hbm, values_hbm, pushed_ref, final_ref, *scratch
):
    halos = scratch[:layers]
    (rows_ref, w_ref, weights_ref, history, features, w_all, weights_t, last_w, values, outgoing, initial, ping, pong, partial,
     load_sem, w_send, w_recv, z_send, z_recv, y_send, y_recv, c_send, c_recv) = scratch[layers:]
    width = w_ref.shape[0]
    nodes = history.shape[1]
    cap = rows_ref.shape[1]
    row_tiles, per_row = values.shape[0], values.shape[1]
    hidden = width * feats
    chips = feats // CORES
    dom = lax.axis_index("dom")
    feat = lax.axis_index("feat")
    chip, core = feat // CORES, feat % CORES
    sibling = chip * CORES + (1 - core)

    half, quarter = doms // 2, doms // 4
    inside = lax.rem(dom // quarter + 1, 4) // 2
    near = [(flips, 0) for flips in range(2, half)]
    outer = [(half + quarter + index, -quarter) for index in range(quarter)]
    inner = [(half + index, quarter) for index in range(quarter)]
    groups = {"X": [(1, 0)], "N": near, "O": outer, "I": inner}

    def chosen(table, index):
        if isinstance(index, int):
            base, slope = table[index]
            return base + slope * inside
        value = 0
        for place, (base, slope) in enumerate(table):
            value = value + jnp.where(index == place, base + slope * inside, 0)
        return value

    def partner(flips):
        dest, bit = dom, 1
        while bit < doms:
            dest = dest + lax.rem(flips // bit, 2) * (bit - 2 * bit * lax.rem(dom // bit, 2))
            bit *= 2
        return dest

    barrier = pltpu.get_barrier_semaphore()
    for step in range(1, doms):
        pl.semaphore_signal(
            barrier, inc=1, device_id={"dom": lax.rem(dom + step, doms)}, device_id_type=MESH
        )
    for step in range(1, feats):
        pl.semaphore_signal(
            barrier, inc=1, device_id={"feat": lax.rem(feat + step, feats)}, device_id_type=MESH
        )
    for hop in range(1, chips):
        across = {"dom": partner(1), "feat": lax.rem(chip + hop, chips) * CORES + core}
        pl.semaphore_signal(barrier, inc=1, device_id=across, device_id_type=MESH)

    rows_load = pltpu.make_async_copy(rows_hbm, rows_ref, load_sem.at[5])
    loads = [
        pltpu.make_async_copy(history_hbm, history, load_sem.at[0]),
        pltpu.make_async_copy(features_hbm, features, load_sem.at[1]),
        pltpu.make_async_copy(values_hbm, values, load_sem.at[2]),
        pltpu.make_async_copy(w_hbm, w_ref, load_sem.at[3]),
        pltpu.make_async_copy(weights_hbm, weights_ref, load_sem.at[4]),
    ]
    for load in (loads[0], rows_load, *loads[1:]):
        load.start()

    def slice_rows(index):
        return pl.ds(pl.multiple_of(index * width, width), width)

    blocks = cap // tile

    def block_tiles(source):
        return pl.ds(source * blocks, blocks)

    def w_copy(step):
        return pltpu.make_async_remote_copy(
            src_ref=w_ref,
            dst_ref=w_all.at[slice_rows(feat)],
            send_sem=w_send.at[step],
            recv_sem=w_recv.at[step],
            device_id={"feat": lax.rem(feat + step, feats)},
            device_id_type=MESH,
        )

    def z_copy(level, flips):
        return pltpu.make_async_remote_copy(
            src_ref=outgoing.at[flips, :, pl.ds(level * width, width)],
            dst_ref=halos[level].at[block_tiles(dom), slice_rows(feat)],
            send_sem=z_send.at[0],
            recv_sem=z_recv.at[level, flips],
            device_id={"dom": partner(flips)},
            device_id_type=MESH,
        )

    def y_copy(level, flips, hop):
        block = halos[level].at[block_tiles(partner(flips)), slice_rows(feat)]
        return pltpu.make_async_remote_copy(
            src_ref=block,
            dst_ref=block,
            send_sem=y_send.at[hop],
            recv_sem=y_recv.at[level, flips, hop],
            device_id={"feat": lax.rem(chip + hop, chips) * CORES + core},
            device_id_type=MESH,
        )

    def x_copy(level, hop):
        return pltpu.make_async_remote_copy(
            src_ref=outgoing.at[1, :, pl.ds(level * width, width)],
            dst_ref=halos[level].at[block_tiles(dom), slice_rows(feat)],
            send_sem=y_send.at[hop],
            recv_sem=y_recv.at[level, 1, hop],
            device_id={"dom": partner(1), "feat": lax.rem(chip + hop, chips) * CORES + core},
            device_id_type=MESH,
        )

    def x_send(level):
        z_copy(level, 1).start()
        for hop in range(1, chips):
            x_copy(level, hop).start()

    def c_copy(level, flips, hop):
        owner = lax.rem(chip + chips - hop, chips) * CORES + core
        block = halos[level].at[block_tiles(partner(flips)), slice_rows(owner)]
        return pltpu.make_async_remote_copy(
            src_ref=block,
            dst_ref=block,
            send_sem=c_send.at[hop],
            recv_sem=c_recv.at[level],
            device_id={"feat": sibling},
            device_id_type=MESH,
        )

    def gather(flips):
        dest = partner(flips)
        part = min(cap, 256)
        for begin in range(0, cap, part):
            slots = begin + lax.broadcasted_iota(jnp.int32, (1, part), 1)
            rows = rows_ref[pl.ds(dest, 1), pl.ds(begin, part)]
            rows = jnp.where(slots < counts_ref[0, dest], rows, -1)
            nodes_iota = lax.broadcasted_iota(jnp.int32, (nodes, part), 0)
            onehot = jnp.where(nodes_iota == rows, 1.0, 0.0).astype(jnp.bfloat16)
            picked = jnp.dot(history[...], onehot, preferred_element_type=jnp.float32)
            picked = picked.astype(jnp.bfloat16)
            for offset in range(0, part, tile):
                outgoing[flips, (begin + offset) // tile] = picked[:, offset : offset + tile]

    def arrive(level, kind, flips, index):
        z_copy(level, flips).wait_recv()
        if kind == "N" and level + 2 < layers:
            z_copy(level + 2, flips).start()
        if level + 1 < layers and kind == PACE_KINDS[level]:

            @pl.when(inside == 0)
            def _():
                z_copy(level + 1, chosen(outer, index)).start()
                z_copy(level + 1, chosen(inner, index)).start()

        if kind != "X":
            for hop in range(1, chips):
                y_copy(level, flips, hop).start()
        elif level + 2 < layers:
            x_send(level + 2)
        c_copy(level, flips, 0).start()

    def relay(level, flips):
        for hop in range(1, chips):
            y_copy(level, flips, hop).wait_recv()
            c_copy(level, flips, hop).start()

    def settle(level):
        span = halos[level].at[pl.ds(0, (doms - 1) * chips * blocks // feats)]
        pltpu.make_async_remote_copy(
            src_ref=span,
            dst_ref=span,
            send_sem=c_send.at[0],
            recv_sem=c_recv.at[level],
            device_id={"feat": sibling},
            device_id_type=MESH,
        ).wait_recv()

    def drain(sem):
        span = outgoing.at[pl.ds(1, doms - 1)]
        pltpu.make_async_remote_copy(
            src_ref=span,
            dst_ref=span,
            send_sem=sem,
            recv_sem=c_recv.at[0],
            device_id={"feat": sibling},
            device_id_type=MESH,
        ).wait_send()

    group = GROUP

    def initial_group(index):
        span = group * tile
        part = pl.ds(pl.multiple_of(index * span, span), span)
        product = lax.dot_general(
            w_all[...], features[part, :], NT, preferred_element_type=jnp.float32
        )
        product = jnp.maximum(product, 0.0).astype(jnp.bfloat16)
        for offset in range(group):
            initial[index * group + offset] = product[:, offset * tile : (offset + 1) * tile]

    states = [initial] + [ping if index % 2 == 0 else pong for index in range(layers - 1)]

    def summed(row, first, last, current, halo):
        picked = []
        for k in range(first, last):
            column = columns_ref[k, row]
            if k < OWN_TILES:
                picked.append(current[column])
            else:
                picked.append(halo[jnp.maximum(column - row_tiles, 0)])
        return lax.dot_general(
            jnp.concatenate(picked, axis=1),
            jnp.concatenate([values[row, k] for k in range(first, last)], axis=1),
            NT,
            preferred_element_type=jnp.float32,
        )

    last = layers - 1

    def own_group(layer, index):
        for offset in range(group):
            row = index * group + offset
            total = summed(row, 0, OWN_TILES, states[layer], None)
            start = initial[row].astype(jnp.float32)
            partial[row] = (1.0 - ALPHA) * total + ALPHA * start
            columns = pl.ds(pl.multiple_of(row * tile, tile), tile)
            pushed_ref[layer, :, columns] = states[layer][row, slice_rows(feat), :]

    def blended_group(layer, index, group=group):
        pieces = []
        for offset in range(group):
            row = index * group + offset
            total = summed(row, OWN_TILES, per_row, None, halos[layer])
            pieces.append((partial[row] + (1.0 - ALPHA) * total).astype(jnp.bfloat16))
        return jnp.concatenate(pieces, axis=1)

    def layer_group(layer, index):
        beta = math.log(LAMBDA_DECAY / (layer + 1) + 1.0)
        following = states[layer + 1]
        blended = blended_group(layer, index)
        product = jnp.dot(weights_t[layer], blended, preferred_element_type=jnp.float32)
        fresh = jnp.maximum((1.0 - beta) * blended.astype(jnp.float32) + beta * product, 0.0)
        fresh = fresh.astype(jnp.bfloat16)
        for offset in range(group):
            following[index * group + offset] = fresh[:, offset * tile : (offset + 1) * tile]

    def last_group(index):
        beta = math.log(LAMBDA_DECAY / layers + 1.0)
        blended = blended_group(last, index, WIDE * group)
        product = jnp.dot(last_w[...], blended, preferred_element_type=jnp.float32)
        fresh = jnp.maximum((1.0 - beta) * product[:width] + beta * product[width:], 0.0)
        fresh = fresh.astype(jnp.bfloat16)
        span = WIDE * group * tile
        final_ref[:, pl.ds(pl.multiple_of(index * span, span), span)] = fresh

    count = row_tiles // group

    def loop(begin, end, body):
        def step(index, carry):
            body(index)
            return carry

        lax.fori_loop(begin, end, step, 0)

    order = [groups[code[0]][int(code[1:])] for code in ORDER]
    rows_load.wait()
    loads[0].wait()
    gather(chosen(order, 0))
    pl.semaphore_wait(barrier, doms + feats + chips - 3)
    if order[0] == (1, 0):
        x_send(0)
        x_send(1)
    else:
        z_copy(0, chosen(order, 0)).start()
    loads[3].wait()
    for step in range(1, feats):
        w_copy(step).start()

    def gather_step(index):
        flips = chosen(order, index)
        gather(flips)
        z_copy(0, flips).start()

    far = [entry for pair in zip(outer, inner) for entry in pair]
    arriving = []
    for code in ARRIVALS:
        level = int(code[1])
        if code[0] in "GH":
            part = far[: half // 2] if code[0] == "G" else far[half // 2 :]
            arriving += [(level, entry, "O" if entry in outer else "I") for entry in part]
        else:
            arriving += [(level, entry, code[0]) for entry in groups[code[0]]]
    early = doms - 1 - EARLY

    cross = order.index((1, 0))

    def gather_span(begin, end):
        if begin <= cross < end:
            loop(begin, cross, gather_step)
            gather(1)
            x_send(0)
            x_send(1)
            begin = cross + 1
        loop(begin, end, gather_step)

    gather_span(1, EARLY)
    for index in range(early):
        gather_span(EARLY + index, EARLY + index + 1)
        level, entry, kind = arriving[index]
        arrive(level, kind, chosen([entry], 0), groups[kind].index(entry))
    loop(0, len(near), lambda index: z_copy(1, chosen(near, index)).start())

    @pl.when(inside == 1)
    def _():
        for level in range(1, layers):
            loop(0, quarter, lambda index: z_copy(level, chosen(outer, index)).start())
            loop(0, quarter, lambda index: z_copy(level, chosen(inner, index)).start())

    loads[4].wait()
    for level in range(layers):
        halos[level][block_tiles(dom)] = jnp.zeros((blocks, hidden, tile), jnp.bfloat16)
        weights_t[level] = weights_ref[level].astype(jnp.float32).T.astype(jnp.bfloat16)
    rows_iota = lax.broadcasted_iota(jnp.int32, (width, hidden), 0)
    columns_iota = lax.broadcasted_iota(jnp.int32, (width, hidden), 1)
    last_w[:width] = jnp.where(rows_iota + feat * width == columns_iota, 1.0, 0.0).astype(jnp.bfloat16)
    last_w[width:] = weights_t[last, slice_rows(feat)]

    w_all[slice_rows(feat), :] = w_ref[...]
    for step in range(1, feats):
        w_copy(step).wait_recv()
    loads[1].wait()

    works = {"initial": initial_group}
    for layer in range(last):
        works["own" + str(layer)] = functools.partial(own_group, layer)
        works["layer" + str(layer)] = functools.partial(layer_group, layer)
    works["own" + str(last)] = functools.partial(own_group, last)
    works["last"] = last_group
    done = {name: 0 for name in works}

    def run(name, pieces):
        begin = done[name]
        done[name] = end = min(begin + pieces, count)
        if name == "last":
            end //= WIDE
        loop(begin, end, works[name])

    final_step = len(arriving) + LAG
    covered = [
        max(place for place, entry in enumerate(arriving) if entry[0] == layer) + LAG + 1
        for layer in range(layers)
    ]

    def before(name):
        if name == "own0":
            loads[2].wait()
        if name.startswith("layer"):
            settle(int(name[5:]))
        if name == "last":
            settle(last)

    pieces = [("initial", 0)] * count
    for layer in range(last):
        pieces += [("own" + str(layer), 0)] * count
        pieces += [("layer" + str(layer), covered[layer] + SLACK)] * count
    pieces += [("own" + str(last), 0)] * count
    plan = []
    for step in range(early, final_step):
        piece = pieces.pop(0)[0] if pieces and pieces[0][1] <= step else None
        plan.append(
            (
                arriving[step] if step < len(arriving) else None,
                arriving[step - LAG] if step >= LAG else None,
                piece,
            )
        )

    def like(entry):
        arrived, relayed, piece = entry
        return (arrived and (arrived[0], arrived[2]), relayed and relayed[0], piece)

    while plan:
        length = 1
        while length < len(plan) and like(plan[length]) == like(plan[0]):
            length += 1
        part, plan = plan[:length], plan[length:]
        arrived, relayed, piece = part[0]
        begin = 0
        if piece:
            begin = done[piece]
            done[piece] += length
            if begin == 0:
                before(piece)

        def body(index, part=part, arrived=arrived, relayed=relayed, piece=piece, begin=begin):
            if arrived:
                table = [entry[0][1] for entry in part]
                place = groups[arrived[2]].index(table[0]) + index
                arrive(arrived[0], arrived[2], chosen(table, index), place)
            if relayed:
                relay(relayed[0], chosen([entry[1][1] for entry in part], index))
            if piece:
                works[piece](begin + index)

        loop(0, length, body)
    for name in [*works]:
        if done[name] < count:
            if done[name] == 0:
                before(name)
            run(name, count)

    for step in range(1, feats):
        w_copy(step).wait_send()
    drain(z_send.at[0])
    for hop in range(1, chips):
        drain(y_send.at[hop])
    for hop in range(chips):
        drain(c_send.at[hop])


def on_device(doms, feats, features, w_input, layer_weights, history, tile_values, tile_columns, send_rows, send_counts):
    layers, nodes, width = history.shape
    row_tiles, per_row, tile, _ = tile_values.shape
    cap = send_rows.shape[2]
    hidden = width * feats
    chips = feats // CORES
    any_spec = pl.BlockSpec(memory_space=pl.ANY)
    smem = pl.BlockSpec(memory_space=pltpu.SMEM)
    bf16 = jnp.bfloat16
    dma = pltpu.SemaphoreType.DMA
    pushed, final = pl.pallas_call(
        functools.partial(kernel, doms, feats, layers, tile),
        out_shape=(
            pltpu.VMEM((layers, width, nodes), bf16),
            pltpu.VMEM((width, nodes), bf16),
        ),
        in_specs=[smem, smem] + [any_spec] * 6,
        out_specs=(pl.BlockSpec(memory_space=pltpu.VMEM), pl.BlockSpec(memory_space=pltpu.VMEM)),
        scratch_shapes=[pltpu.VMEM((doms * cap // tile, hidden, tile), bf16) for _ in range(layers)] + [
            pltpu.VMEM(send_rows.shape[1:], jnp.int32),
            pltpu.VMEM((width, features.shape[1]), bf16),
            pltpu.VMEM(layer_weights.shape, bf16),
            pltpu.VMEM((layers * width, nodes), bf16),
            pltpu.VMEM(features.shape, bf16),
            pltpu.VMEM((hidden, features.shape[1]), bf16),
            pltpu.VMEM((layers, hidden, hidden), bf16),
            pltpu.VMEM((2 * width, hidden), bf16),
            pltpu.VMEM(tile_values.shape, bf16),
            pltpu.VMEM((doms, cap // tile, layers * width, tile), bf16),
            pltpu.VMEM((row_tiles, hidden, tile), bf16),
            pltpu.VMEM((row_tiles, hidden, tile), bf16),
            pltpu.VMEM((row_tiles, hidden, tile), bf16),
            pltpu.VMEM((row_tiles, hidden, tile), jnp.float32),
            dma((6,)),
            dma((feats,)),
            dma((feats,)),
            dma((1,)),
            dma((layers, doms)),
            dma((chips,)),
            dma((layers, doms, chips)),
            dma((chips,)),
            dma((layers,)),
        ],
        compiler_params=pltpu.CompilerParams(
            collective_id=0, has_side_effects=True, vmem_limit_bytes=67043328 - 2 * (layers + 1) * width * nodes
        ),
    )(
        tile_columns.T,
        send_counts,
        send_rows[0],
        jnp.swapaxes(history, 1, 2).reshape(layers * width, nodes),
        features,
        w_input.T,
        layer_weights,
        tile_values,
    )
    return jnp.swapaxes(pushed, 1, 2), final.T


def solution(mesh):
    placed = (
        P("dom", None),
        P(None, "feat"),
        P(),
        P(None, "dom", "feat"),
        P("dom", None, None, None),
        P("dom", None),
        P("dom", None, None),
        P("dom", None),
    )
    return jax.shard_map(
        functools.partial(on_device, mesh.shape["dom"], mesh.shape["feat"]),
        mesh=mesh,
        in_specs=placed,
        out_specs=(P(None, "dom", "feat"), P("dom", "feat")),
        check_vma=False,
    )
```
